128 devices in a mesh: dp: 8 (over x, core), mp: 16 (over z, y).
Axes of the slice: x: 4, y: 4, z: 4, core: 2. Of those that a mesh axis runs over, the one named last changes fastest.
Arguments:
- tokens: bfloat16 [2048, 8192], P('dp'), may hold values from -6 to 6
- norm_gain: float32 [8192], replicated, may hold values from 0.5 to 1.5
- gate_weight: bfloat16 [8192, 28672], P('dp', 'mp'), may hold values from -0.0625 to 0.0625
- gate_mask: int32 [8192, 896], P('dp', 'mp'), may hold values from -2147483648 to 2147483646
- up_weight: bfloat16 [8192, 28672], P('dp', 'mp'), may hold values from -0.0625 to 0.0625
- up_mask: int32 [8192, 896], P('dp', 'mp'), may hold values from -2147483648 to 2147483646
- down_weight: bfloat16 [28672, 8192], P('mp', 'dp'), may hold values from -0.03125 to 0.03125
- down_mask: int32 [28672, 256], P('mp', 'dp'), may hold values from -2147483648 to 2147483647, as said below
Outputs:
- mixed: bfloat16 [2048, 8192], P('mp', 'dp')
- input_norms: float32 [8192], P('dp')
- hidden_norms: float32 [28672], P('mp')
The draws below stay inside these ranges and needn't reach their ends.
Inputs may be any that keep to these rules, and one draw needn't show every extreme that they name: `down_mask`: in every word each of the eight aligned groups of four bits holds exactly two ones, so exactly two of every four consecutive columns of the down projection are kept.
All inputs are finite; a program needn't handle non-finite values.
Results may differ from the reference program's by a relative error of at most 0.025.
Values may be sent and summed in bfloat16 or wider, within the bound.
No kernel may reach another device: no remote copies, remote signals or barrier semaphores. Data moves between devices by JAX's collectives and lax.ppermute only.
A program may use at most 128 MiB of HBM per device.

```python
import jax
import jax.numpy as jnp
from jax import lax

D = 8192
FF = 28672
TOKENS = 2048
N_DP = 8
N_MP = 16


def draw_down_mask(key, part):
    patterns = jnp.array([3, 5, 6, 9, 10, 12], jnp.int32)
    selected = jax.random.randint(key, (FF, D // 32, 8), 0, 6, dtype=jnp.int32)
    nibbles = patterns[selected]
    shifts = 4 * jnp.arange(8, dtype=jnp.int32)
    placed = jnp.left_shift(nibbles, shifts)
    return jnp.sum(placed, axis=2, dtype=jnp.int32)


def set_ends(entries, rng, least, largest):
    longest = entries.shape.index(max(entries.shape))
    spots = []
    for shift in (0, 1):
        where = [jax.random.randint(jax.random.fold_in(rng, axis), (), 0, length) for axis, length in enumerate(entries.shape)]
        where[longest] = (where[longest] + shift) % entries.shape[longest]
        spots.append(tuple(where))
    return entries.at[spots[0]].set(least).at[spots[1]].set(largest)


def level_of(key, shape, split, smallest, high):
    def one(axis_at, blocks):
        heights = jax.random.uniform(jax.random.fold_in(jax.random.fold_in(key, 6), axis_at), (blocks,), jnp.float32, smallest / len(split), high / len(split))
        return jnp.repeat(jnp.exp(heights), shape[axis_at] // blocks).reshape((-1,) + (1,) * (len(shape) - axis_at - 1))

    level = one(*split[0])
    for cut in split[1:]:
        level = level * one(*cut)
    return level


def centred(stream_key, extent, width, most, cuts=(), kind=jnp.bfloat16):
    gain = level_of(stream_key, extent, cuts, -0.22, 0.18) if cuts else 1.0
    entries = jax.random.normal(stream_key, extent, jnp.float32) * width * gain
    return jnp.minimum(jnp.maximum(entries, -most), most).astype(kind)


def setup_inputs(seed: int = 0) -> dict:
    keys = jax.random.split(jax.random.key(seed), 9)
    tokens = centred(keys[0], (TOKENS, D), 1.0, 6.0, ((0, 8),))
    norm_gain = jnp.clip(1.0 + 0.1 * jax.random.normal(keys[1], (D,), jnp.float32), 0.5, 1.5)
    gate_weight = centred(keys[2], (D, FF), D ** -0.5, 0.0625, ((0, 8), (1, 16)))
    gate_mask = set_ends(jax.random.randint(keys[3], (D, FF // 32), -2147483648, 2147483647), jax.random.fold_in(keys[3], 1), -2147483648, 2147483646).astype(jnp.int32)
    up_weight = centred(keys[4], (D, FF), D ** -0.5, 0.0625, ((0, 8), (1, 16)))
    up_mask = set_ends(jax.random.randint(keys[5], (D, FF // 32), -2147483648, 2147483647), jax.random.fold_in(keys[5], 1), -2147483648, 2147483646).astype(jnp.int32)
    down_weight = centred(keys[6], (FF, D), FF ** -0.5, 0.03125, ((0, 16), (1, 8)))
    down_mask = draw_down_mask(jax.random.fold_in(keys[8], 71), 0)
    return dict(tokens=tokens, norm_gain=norm_gain, gate_weight=gate_weight, gate_mask=gate_mask, up_weight=up_weight, up_mask=up_mask, down_weight=down_weight, down_mask=down_mask)


def keep_entries(weight, packed):
    shifts = jnp.arange(32, dtype=jnp.int32)
    kept_bits = jnp.right_shift(packed[..., None], shifts) & 1
    kept_bits = kept_bits.reshape(weight.shape)
    return jnp.where(kept_bits == 1, weight, jnp.zeros_like(weight))

def reference(tokens, norm_gain, gate_weight, gate_mask, up_weight, up_mask, down_weight, down_mask):
    values = tokens.astype(jnp.float32)
    scale = lax.rsqrt(lax.optimization_barrier(jnp.mean(values * values, axis=1, keepdims=True)) + 1e-05)
    normed = (values * scale * norm_gain).astype(jnp.bfloat16)
    widened = normed.astype(jnp.float32)
    input_norms = jnp.sqrt(lax.optimization_barrier(jnp.sum(widened * widened, axis=0)))
    stride = D // N_DP

    def add_block(position, sums_so_far):
        gate_sum, up_sum = sums_so_far
        offset = (position * stride).astype(jnp.int32)
        row_block = lax.dynamic_slice_in_dim(normed, offset, stride, 1)
        gate_rows = keep_entries(lax.dynamic_slice_in_dim(gate_weight, offset, stride, 0), lax.dynamic_slice_in_dim(gate_mask, offset, stride, 0))
        up_rows = keep_entries(lax.dynamic_slice_in_dim(up_weight, offset, stride, 0), lax.dynamic_slice_in_dim(up_mask, offset, stride, 0))
        gate_part = jnp.dot(row_block, gate_rows, preferred_element_type=jnp.float32).astype(jnp.bfloat16)
        up_part = jnp.dot(row_block, up_rows, preferred_element_type=jnp.float32).astype(jnp.bfloat16)
        gate_part, up_part = lax.optimization_barrier((gate_part, up_part))
        return (gate_sum + gate_part.astype(jnp.float32), up_sum + up_part.astype(jnp.float32))
    zeros_sum = jnp.zeros((normed.shape[0], FF), jnp.float32)
    gate, up = lax.fori_loop(0, N_DP, add_block, (zeros_sum, zeros_sum))
    hidden = (jax.nn.silu(gate) * up).astype(jnp.bfloat16)
    wide_hidden = hidden.astype(jnp.float32)
    hidden_norms = jnp.sqrt(lax.optimization_barrier(jnp.sum(wide_hidden * wide_hidden, axis=0)))
    unit_stride = FF // N_MP

    def add_down(position, running):
        offset = (position * unit_stride).astype(jnp.int32)
        row_block = lax.dynamic_slice_in_dim(hidden, offset, unit_stride, 1)
        down_rows = keep_entries(lax.dynamic_slice_in_dim(down_weight, offset, unit_stride, 0), lax.dynamic_slice_in_dim(down_mask, offset, unit_stride, 0))
        return running + jnp.dot(row_block, down_rows, preferred_element_type=jnp.float32)
    mixed = lax.fori_loop(0, N_MP, add_down, jnp.zeros((normed.shape[0], D), jnp.float32))
    return (mixed.astype(jnp.bfloat16), input_norms, hidden_norms)
```

```python
import jax
import jax.numpy as jnp
from jax import lax
from jax.experimental import pallas as pl
from jax.experimental.pallas import tpu as pltpu
from jax.sharding import Mesh
from jax.sharding import PartitionSpec as P

DP = ("x", "c")
MP = ("z", "y")
BF = jnp.bfloat16
F32 = jnp.float32
CHUNKS = 2
VMEM = pl.BlockSpec(memory_space=pltpu.VMEM)
SMEM = pl.BlockSpec(memory_space=pltpu.SMEM)


def params():
    return pltpu.CompilerParams(vmem_limit_bytes=50 * 1024 * 1024)


def cost(flops, nbytes):
    return pl.CostEstimate(flops=int(flops), bytes_accessed=int(nbytes), transcendentals=0)


def shift(array, axis, by):
    size = lax.axis_size(axis)
    return lax.ppermute(array, axis, [(i, (i + by) % size) for i in range(size)])


def swap(array):
    return lax.ppermute(array, "c", [(0, 1), (1, 0)])


def norm_call(idx, tokens, gain):
    rows, width = tokens.shape
    nx = 4
    part = width // nx
    group = rows // (2 * CHUNKS)
    piece = group // 4

    def body(idx_ref, tok_ref, gain_ref, own_ref, *send_refs):
        x = idx_ref[0]

        def scaled(values, scale, d):
            start = pl.multiple_of(lax.rem(x + d, nx) * part, part)
            g = gain_ref[:, pl.ds(start, part)]
            return start, g

        for k in range(CHUNKS):
            for h in range(2):
                base = h * (rows // 2) + k * group
                v = tok_ref[pl.ds(base, group), :].astype(F32)
                scale = lax.rsqrt(jnp.mean(v * v, axis=1, keepdims=True) + 1e-05)
                start, g = scaled(None, None, 0)
                own = tok_ref[pl.ds(base, group), pl.ds(start, part)].astype(F32)
                own_ref[k, pl.ds(h * group, group), :] = (own * scale * g).astype(BF)
                pick = idx_ref[2 + h]
                at = pl.multiple_of(base + pick * piece, piece)
                v = tok_ref[pl.ds(at, piece), :].astype(F32)
                scale = lax.rsqrt(jnp.mean(v * v, axis=1, keepdims=True) + 1e-05)
                for d in range(1, nx):
                    start, g = scaled(None, None, d)
                    sent = tok_ref[pl.ds(at, piece), pl.ds(start, part)].astype(F32)
                    send_refs[k * 3 + d - 1][h] = (sent * scale * g).astype(BF)

    out = [jax.ShapeDtypeStruct((CHUNKS, 2 * group, part), BF)]
    out += [jax.ShapeDtypeStruct((2, piece, part), BF)] * (3 * CHUNKS)
    res = pl.pallas_call(
        body,
        out_shape=out,
        in_specs=[SMEM, VMEM, VMEM],
        out_specs=[VMEM] * len(out),
        compiler_params=params(),
        cost_estimate=cost(2e9, 8e6),
        name="norm",
    )(idx, tokens, gain.reshape(1, width))
    return res[0], [res[1 + 3 * k : 4 + 3 * k] for k in range(CHUNKS)]


def spread(mask_t, columns, words):
    parts = [jnp.bitwise_and(jnp.right_shift(mask_t, 8 * b), 255) for b in range(4)]
    stacked = jnp.concatenate([p.astype(F32) for p in parts], axis=0).astype(BF)
    return lax.dot_general(
        stacked, columns, (((0,), (0,)), ((), ())), preferred_element_type=F32
    ).astype(jnp.int32)


def fill_onehot(ref, words):
    q = lax.broadcasted_iota(jnp.int32, ref.shape, 0)
    c = lax.broadcasted_iota(jnp.int32, ref.shape, 1)
    hit = jnp.logical_and(
        lax.rem(q, words) == lax.div(c, 32), lax.div(q, words) == lax.div(lax.rem(c, 32), 8)
    )
    ref[...] = jnp.where(hit, 1.0, 0.0).astype(BF)


def kept(weight, spread_bytes):
    c = lax.broadcasted_iota(jnp.int32, (1, weight.shape[1]), 1)
    bit = jnp.left_shift(1, jnp.bitwise_and(c, 7))
    on = jnp.bitwise_and(spread_bytes, bit) != 0
    return jnp.where(on, weight.astype(F32), 0.0).astype(BF)


def mask_pair(idx, gate, gate_mask, up, up_mask):
    rows, units = gate.shape
    words = gate_mask.shape[1]
    half = units // 2
    step = 256

    def body(idx_ref, g_ref, gm_ref, u_ref, um_ref, keep_ref, send_ref, hot_ref):
        @pl.when(pl.program_id(0) == 0)
        def _():
            fill_onehot(hot_ref, words)

        c = idx_ref[1]
        for which, out_ref in ((c, keep_ref), (1 - c, send_ref)):
            cols = pl.ds(pl.multiple_of(which * half, 128), half)
            hot = hot_ref[:, cols]
            out_ref[:, :half] = kept(g_ref[:, cols], spread(gm_ref[...], hot, words))
            out_ref[:, half:] = kept(u_ref[:, cols], spread(um_ref[...], hot, words))

    wide = pl.BlockSpec((step, units), lambda i: (i, 0))
    thin = pl.BlockSpec((words, step), lambda i: (0, i))
    return pl.pallas_call(
        body,
        out_shape=[jax.ShapeDtypeStruct((rows, units), BF)] * 2,
        grid=(rows // step,),
        in_specs=[SMEM, wide, thin, wide, thin],
        out_specs=[wide, wide],
        scratch_shapes=[pltpu.VMEM((4 * words, units), BF)],
        compiler_params=params(),
        cost_estimate=cost(4e9, 16e6),
        name="mask_pair",
    )(idx, gate, gate_mask.T, up, up_mask.T)


def mask_one(weight, mask):
    rows, cols = weight.shape
    words = mask.shape[1]
    step = 256

    def body(w_ref, m_ref, out_ref, hot_ref):
        @pl.when(pl.program_id(0) == 0)
        def _():
            fill_onehot(hot_ref, words)

        out_ref[...] = kept(w_ref[...], spread(m_ref[...], hot_ref[...], words))

    wide = pl.BlockSpec((step, cols), lambda i: (i, 0))
    return pl.pallas_call(
        body,
        out_shape=jax.ShapeDtypeStruct((rows, cols), BF),
        grid=(rows // step,),
        in_specs=[wide, pl.BlockSpec((words, step), lambda i: (0, i))],
        out_specs=wide,
        scratch_shapes=[pltpu.VMEM((4 * words, cols), BF)],
        compiler_params=params(),
        cost_estimate=cost(2e9, 8e6),
        name="mask_one",
    )(weight, mask.T)


def assemble(idx, by_z, by_y):
    three, piece, width = by_z[0].shape
    half = 4 * piece

    def body(idx_ref, *refs):
        out_ref = refs[-1]
        for h in range(2):
            for e in range(4):
                slot = lax.rem(idx_ref[2 + h] + 4 - e, 4)
                at = pl.multiple_of(h * half + slot * piece, piece)
                for d in range(three):
                    out_ref[d, pl.ds(at, piece), :] = refs[h * 4 + e][d]

    return pl.pallas_call(
        body,
        out_shape=jax.ShapeDtypeStruct((three, 2 * half, width), BF),
        in_specs=[SMEM] + [VMEM] * 8,
        out_specs=VMEM,
        compiler_params=params(),
        cost_estimate=cost(1e8, 3e6),
        name="assemble",
    )(idx, *by_z, *by_y)


def product(idx, mine, theirs, at, w_own, w_recv, add=None, add_to=None, wide=False):
    rows, feats = mine.shape[1:]
    part, cols = w_own.shape
    tile = 256

    def body(idx_ref, a_ref, b_ref, wo_ref, wr_ref, *rest):
        c = idx_ref[1]
        first = pl.ds(pl.multiple_of(c * part, part), part)
        second = pl.ds(pl.multiple_of((1 - c) * part, part), part)
        acc = jnp.dot(
            jnp.concatenate([a_ref[0, :, first], b_ref[0, :, first]], axis=0),
            wo_ref[...],
            preferred_element_type=F32,
        )
        acc += jnp.dot(
            jnp.concatenate([a_ref[0, :, second], b_ref[0, :, second]], axis=0),
            wr_ref[...],
            preferred_element_type=F32,
        )
        sums = [acc[:rows], acc[rows:]]
        if add is not None:
            sums[add_to] += rest[0][...].astype(F32)
        if wide == "split":
            rest[-2][...] = sums[0].astype(BF)
            rest[-1][...] = sums[1].astype(BF)
        else:
            rest[-1][0] = sums[0].astype(rest[-1].dtype)
            rest[-1][1] = sums[1].astype(rest[-1].dtype)

    x_spec = pl.BlockSpec((1, rows, feats), lambda j: (at, 0, 0))
    w_spec = pl.BlockSpec((part, tile), lambda j: (0, j))
    flat = pl.BlockSpec((rows, tile), lambda j: (0, j))
    both = pl.BlockSpec((2, rows, tile), lambda j: (0, 0, j))
    ins = [SMEM, x_spec, x_spec, w_spec, w_spec] + ([flat] if add is not None else [])
    args = [idx, mine, theirs, w_own, w_recv] + ([add] if add is not None else [])
    if wide == "split":
        out_shape = [jax.ShapeDtypeStruct((rows, cols), BF)] * 2
        out_specs = [flat, flat]
    else:
        out_shape = jax.ShapeDtypeStruct((2, rows, cols), F32 if wide else BF)
        out_specs = both
    return pl.pallas_call(
        body,
        out_shape=out_shape,
        grid=(cols // tile,),
        in_specs=ins,
        out_specs=out_specs,
        compiler_params=params(),
        cost_estimate=cost(4 * rows * feats * cols, 1e7),
        name="product",
    )(*args)


def hidden_call(own, left, right):
    two, rows, cols = own.shape
    units = cols // 2

    def body(o_ref, l_ref, r_ref, out_ref, sq_ref):
        total = jnp.zeros((1, units), F32)
        for h in range(two):
            def both(cut):
                return (
                    o_ref[h, :, cut] + l_ref[h, :, cut].astype(F32) + r_ref[h, :, cut].astype(F32)
                )

            gate = both(slice(0, units))
            up = both(slice(units, cols))
            hid = (gate / (1.0 + jnp.exp(-gate)) * up).astype(BF)
            out_ref[h] = hid
            w = hid.astype(F32)
            total += jnp.sum(w * w, axis=0, keepdims=True)
        sq_ref[...] = total

    return pl.pallas_call(
        body,
        out_shape=[
            jax.ShapeDtypeStruct((two, rows, units), BF),
            jax.ShapeDtypeStruct((1, units), F32),
        ],
        in_specs=[VMEM] * 3,
        out_specs=[VMEM] * 2,
        compiler_params=params(),
        cost_estimate=cost(1e9, 4e6),
        name="hidden",
    )(own, left, right)


def down_call(idx, own_cols, their_cols, weight):
    rows, units = own_cols[3].shape
    cols = weight.shape[1]
    half = cols // 2
    quarter = rows // 2

    def body(idx_ref, h0, h1, h3, h2a, h2b, p0, p1, p3, p2a, p2b, w_ref, oz_ref, oy_ref):
        x = idx_ref[0]
        c = idx_ref[1]
        w_own = w_ref[pl.ds(pl.multiple_of(c * units, 128), units), :]
        w_other = w_ref[pl.ds(pl.multiple_of((1 - c) * units, 128), units), :]
        sets = [
            (0, (h0[0], h0[1]), (p0[1], p0[0])),
            (1, (h1[0], h1[1]), (p1[1], p1[0])),
            (3, (h3[0], h3[1]), (p3[1], p3[0])),
            (2, (h2a[...], h2b[...]), (p2b[...], p2a[...])),
        ]
        for d, mine, theirs in sets:
            acc = jnp.dot(jnp.concatenate(mine, axis=0), w_own, preferred_element_type=F32)
            acc += jnp.dot(jnp.concatenate(theirs, axis=0), w_other, preferred_element_type=F32)
            out = acc.astype(BF)
            z = lax.rem(x + 4 - d, 4)
            for s, core in ((0, c), (1, 1 - c)):
                for h in range(2):
                    y = 2 * core + h
                    lo = s * rows + h * quarter
                    oz_ref[z, y] = out[lo : lo + quarter, :half]
                    oy_ref[y, z] = out[lo : lo + quarter, half:]

    return pl.pallas_call(
        body,
        out_shape=[jax.ShapeDtypeStruct((4, 4, quarter, half), BF)] * 2,
        in_specs=[SMEM] + [VMEM] * 11,
        out_specs=[VMEM] * 2,
        compiler_params=params(),
        cost_estimate=cost(4e9, 8e6),
        name="down",
    )(idx, *own_cols, *their_cols, weight)


def column_squares(idx, arrays):
    part = arrays[0].shape[2] // 2

    def body(*refs):
        total = jnp.zeros((8, part), F32)
        for ref in refs[1:-1]:
            for i in range(ref.shape[0]):
                v = ref[i].astype(F32)
                v = (v * v).reshape(-1, 8, part)
                total += jnp.sum(v, axis=0)
        refs[-1][...] = jnp.sum(total, axis=0, keepdims=True)

    def spec(a):
        return pl.BlockSpec((a.shape[0], a.shape[1], part), lambda i, idx_ref: (0, 0, idx_ref[1]))

    return pl.pallas_call(
        lambda *refs: body(*refs),
        out_shape=jax.ShapeDtypeStruct((1, part), F32),
        grid_spec=pltpu.PrefetchScalarGridSpec(
            num_scalar_prefetch=1,
            grid=(1,),
            in_specs=[spec(a) for a in arrays],
            out_specs=pl.BlockSpec((1, part), lambda i, idx_ref: (0, 0)),
        ),
        compiler_params=params(),
        cost_estimate=cost(1e9, 4e6),
        name="squares",
    )(idx, *arrays)


def summed(parts):
    return jnp.sum(parts.astype(F32), axis=0).astype(BF)


def on_device(
    tokens, norm_gain, gate_weight, gate_mask, up_weight, up_mask, down_weight, down_mask
):
    idx = jnp.stack([lax.axis_index(a) for a in ("x", "c", "z", "y")]).astype(jnp.int32)
    own_x, sends = norm_call(idx, tokens, norm_gain)
    got = [[shift(s[d - 1], "x", d) for d in (1, 2, 3)] for s in sends]
    own_theirs = swap(own_x)
    w_own, w_send = mask_pair(idx, gate_weight, gate_mask, up_weight, up_mask)
    w_recv = swap(w_send)
    mine, theirs = [], []
    for k in range(CHUNKS):
        stacked = jnp.stack(got[k])
        zs, ys = stacked[:, 0], stacked[:, 1]
        by_z = [zs] + [shift(zs, "z", e) for e in (1, 2, 3)]
        by_y = [ys] + [shift(ys, "y", e) for e in (1, 2, 3)]
        mine.append(assemble(idx, by_z, by_y))
        theirs.append(swap(mine[k]))
    down_kept = mask_one(down_weight, down_mask)

    first = []
    for k in range(CHUNKS):
        a, b = product(idx, mine[k], theirs[k], 1, w_own, w_recv, wide="split")
        first.append((shift(a, "x", 1), shift(b, "x", 3)))
    own_part = [product(idx, own_x, own_theirs, k, w_own, w_recv, wide=True) for k in range(CHUNKS)]
    hid, squares = [], 0.0
    for k in range(CHUNKS):
        from_left, from_right = first[k]
        ahead = product(idx, mine[k], theirs[k], 2, w_own, w_recv, from_left, 0)
        behind = product(idx, mine[k], theirs[k], 0, w_own, w_recv, from_right, 1)
        left = shift(ahead, "x", 1)
        right = shift(behind, "x", 3)
        h, sq = hidden_call(own_part[k], left, right)
        hid.append(h)
        squares = squares + sq
    outs = []
    for k in range(CHUNKS):
        h0 = hid[k]
        h1 = shift(h0, "x", 1)
        h3 = shift(h0, "x", 3)
        h2a = shift(h1[0], "x", 1)
        h2b = shift(h3[1], "x", 3)
        own_cols = (h0, h1, h3, h2a, h2b)
        oz, oy = down_call(idx, own_cols, [swap(h) for h in own_cols], down_kept)
        az = summed(lax.all_to_all(oz, "z", 0, 0, tiled=True))
        ay = summed(lax.all_to_all(oy, "y", 0, 0, tiled=True))
        bz = summed(lax.all_to_all(az, "y", 0, 0, tiled=True))
        by = summed(lax.all_to_all(ay, "z", 0, 0, tiled=True))
        outs.append(jnp.concatenate([bz, by], axis=1))
    mixed = jnp.concatenate(outs, axis=0)

    input_norms = jnp.sqrt(column_squares(idx, [own_x, own_theirs, *mine, *theirs])[0])
    every = lax.all_to_all(
        jnp.broadcast_to(squares[None], (8, 1, squares.shape[1])), DP, 0, 0, tiled=True
    )
    hidden_norms = jnp.sqrt(jnp.sum(every.reshape(4, -1), axis=0))
    return (mixed, input_norms, hidden_norms)


def solution(mesh):
    finer = Mesh(mesh.devices.reshape(4, 2, 4, 4), DP + MP)
    in_specs = (
        P(DP, None),
        P(),
        P(DP, MP),
        P(DP, MP),
        P(DP, MP),
        P(DP, MP),
        P(MP, DP),
        P(MP, DP),
    )
    out_specs = (P(MP, DP), P(DP), P(MP))
    return jax.shard_map(
        on_device, mesh=finer, in_specs=in_specs, out_specs=out_specs, check_vma=False
    )
```

```python
import jax
import jax.numpy as jnp
from jax import lax
from jax.experimental import pallas as pl
from jax.experimental.pallas import tpu as pltpu
from jax.sharding import Mesh
from jax.sharding import PartitionSpec as P

DP = ("x", "c")
MP = ("z", "y")
BF = jnp.bfloat16
F32 = jnp.float32
SPLIT = (64, 64)
FULL_TILE = 1792
SMALL_TILE = 256
DOWN_TILE = 512
MASK_ROWS = 128

VMEM = pl.BlockSpec(memory_space=pltpu.VMEM)
SMEM = pl.BlockSpec(memory_space=pltpu.SMEM)
HBM = pl.BlockSpec(memory_space=pltpu.HBM)


def params(mib=24):
    return pltpu.CompilerParams(vmem_limit_bytes=mib * 1024 * 1024)


def in_hbm(array):
    return pltpu.with_memory_space_constraint(array, pltpu.HBM)


def in_vmem(array):
    return pltpu.with_memory_space_constraint(array, pltpu.VMEM)


def cost(flops, nbytes):
    return pl.CostEstimate(flops=int(flops), bytes_accessed=int(nbytes), transcendentals=0)


def shift(array, axis, by):
    size = lax.axis_size(axis)
    return lax.ppermute(array, axis, [(i, (i + by) % size) for i in range(size)])


def swap(array):
    return lax.ppermute(array, "c", [(0, 1), (1, 0)])


def norm_call(idx, tokens, gain, dists, which=None):
    rows, width = tokens.shape
    nx = 4
    part = width // nx
    block = rows // 4
    steps = 4 if which is None else 1

    def body(idx_ref, tok_hbm, gain_hbm, *rest):
        out_refs = rest[: len(dists)]
        tok_ref, gain_ref, sems = rest[len(dists) :]
        copies = [pltpu.make_async_copy(gain_hbm, gain_ref, sems.at[steps])]
        for i in range(steps):
            at = i * block if which is None else pl.multiple_of(idx_ref[which] * block, block)
            src = tok_hbm.at[pl.ds(at, block), :]
            copies.append(pltpu.make_async_copy(src, tok_ref.at[i], sems.at[i]))
        for copy in copies:
            copy.start()
        copies[0].wait()
        for i in range(steps):
            copies[1 + i].wait()
            v = tok_ref[i].astype(F32)
            scale = lax.rsqrt(jnp.mean(v * v, axis=1, keepdims=True) + 1e-05)
            for d, out_ref in zip(dists, out_refs):
                cut = pl.ds(pl.multiple_of(lax.rem(idx_ref[0] + d, nx) * part, part), part)
                v = tok_ref[i, :, cut].astype(F32)
                out_ref[i * block : (i + 1) * block] = (v * scale * gain_ref[:, cut]).astype(BF)

    return pl.pallas_call(
        body,
        out_shape=[jax.ShapeDtypeStruct((steps * block, part), BF)] * len(dists),
        in_specs=[SMEM, HBM, HBM],
        out_specs=[VMEM] * len(dists),
        scratch_shapes=[
            pltpu.VMEM((steps, block, width), BF),
            pltpu.VMEM((1, width), F32),
            pltpu.SemaphoreType.DMA((steps + 1,)),
        ],
        compiler_params=params(10),
        cost_estimate=cost(5e8 * steps, 2e6 * steps),
        name="norm",
    )(idx, in_hbm(tokens), in_hbm(gain.reshape(1, width)))


def spread(mask_t, columns):
    parts = [jnp.bitwise_and(jnp.right_shift(mask_t, 8 * b), 255) for b in range(4)]
    stacked = jnp.concatenate([p.astype(F32) for p in parts], axis=0).astype(BF)
    return lax.dot_general(
        stacked, columns, (((0,), (0,)), ((), ())), preferred_element_type=F32
    ).astype(jnp.int32)


def fill_onehot(ref, words):
    q = lax.broadcasted_iota(jnp.int32, ref.shape, 0)
    c = lax.broadcasted_iota(jnp.int32, ref.shape, 1)
    hit = jnp.logical_and(
        lax.rem(q, words) == lax.div(c, 32), lax.div(q, words) == lax.div(lax.rem(c, 32), 8)
    )
    ref[...] = jnp.where(hit, 1.0, 0.0).astype(BF)


def kept(weight, spread_bytes):
    c = lax.broadcasted_iota(jnp.int32, (1, weight.shape[1]), 1)
    bit = jnp.left_shift(1, jnp.bitwise_and(c, 7))
    on = jnp.bitwise_and(spread_bytes, bit) != 0
    return jnp.where(on, weight.astype(F32), 0.0).astype(BF)


def mask_pair(idx, gate, gate_mask, up, up_mask):
    rows, units = gate.shape
    words = gate_mask.shape[1]
    half = units // 2
    step = MASK_ROWS

    def body(idx_ref, g_ref, gm_ref, u_ref, um_ref, keep_ref, send_ref, hot_ref):
        @pl.when(pl.program_id(0) == 0)
        def _():
            fill_onehot(hot_ref, words)

        c = idx_ref[1]
        for which, out_ref in ((c, keep_ref), (1 - c, send_ref)):
            cols = pl.ds(pl.multiple_of(which * half, 128), half)
            hot = hot_ref[:, cols]
            out_ref[:, :half] = kept(g_ref[:, cols], spread(gm_ref[...], hot))
            out_ref[:, half:] = kept(u_ref[:, cols], spread(um_ref[...], hot))

    wide = pl.BlockSpec((step, units), lambda i: (i, 0))
    thin = pl.BlockSpec((words, step), lambda i: (0, i))
    return pl.pallas_call(
        body,
        out_shape=[jax.ShapeDtypeStruct((rows, units), BF)] * 2,
        grid=(rows // step,),
        in_specs=[SMEM, wide, thin, wide, thin],
        out_specs=[wide, wide],
        scratch_shapes=[pltpu.VMEM((4 * words, units), BF)],
        compiler_params=params(16),
        cost_estimate=cost(4e9, 16e6),
        name="mask_pair",
    )(idx, gate, gate_mask.T, up, up_mask.T)


def mask_one(weight, mask):
    rows, cols = weight.shape
    words = mask.shape[1]
    step = MASK_ROWS

    def body(w_ref, m_ref, out_ref, hot_ref):
        @pl.when(pl.program_id(0) == 0)
        def _():
            fill_onehot(hot_ref, words)

        out_ref[...] = kept(w_ref[...], spread(m_ref[...], hot_ref[...]))

    wide = pl.BlockSpec((step, cols), lambda i: (i, 0))
    return pl.pallas_call(
        body,
        out_shape=pltpu.VMEM((rows, cols), BF),
        grid=(rows // step,),
        in_specs=[wide, pl.BlockSpec((words, step), lambda i: (0, i))],
        out_specs=wide,
        scratch_shapes=[pltpu.VMEM((4 * words, cols), BF)],
        compiler_params=params(10),
        cost_estimate=cost(2e9, 8e6),
        name="mask_one",
    )(weight, mask.T)


def assemble(idx, axis, pieces):
    deep = pieces[0].ndim == 3
    count = pieces[0].shape[0] if deep else 1
    block, width = pieces[0].shape[-2:]

    def body(idx_ref, *refs):
        out_ref = refs[-1]
        for e in range(4):
            slot = lax.rem(idx_ref[axis] + 4 - e, 4)
            to = pl.ds(pl.multiple_of(slot * block, block), block)
            for d in range(count):
                out_ref[d, to, :] = refs[e][d] if deep else refs[e][...]

    return pl.pallas_call(
        body,
        out_shape=jax.ShapeDtypeStruct((count, 4 * block, width), BF),
        in_specs=[SMEM] + [VMEM] * 4,
        out_specs=VMEM,
        compiler_params=params(10),
        cost_estimate=cost(1e8, 3e6),
        name="assemble",
    )(idx, *pieces)


def product(idx, k, tile, groups, w_own, w_recv, adds=()):
    tokens, feats = groups[0][0].shape[1:]
    part, cols = w_own.shape
    skip, count = sum(SPLIT[:k]), SPLIT[k]
    rows = 2 * count

    def body(idx_ref, a_ref, b_ref, wo_ref, wr_ref, *rest):
        c = idx_ref[1]
        lhs_ref = rest[-1]
        for i, ref in ((0, a_ref), (1, b_ref)):
            for h in range(2):
                to = i * rows + h * count
                take = pl.ds(h * (tokens // 2) + skip, count)
                for j, core in ((0, c), (1, 1 - c)):
                    lhs_ref[to : to + count, j * part : (j + 1) * part] = ref[
                        0, take, pl.ds(pl.multiple_of(core * part, part), part)
                    ]

        def columns(j, carry):
            cut = pl.ds(pl.multiple_of(j * tile, tile), tile)
            acc = jnp.dot(lhs_ref[:, :part], wo_ref[:, cut], preferred_element_type=F32)
            acc += jnp.dot(lhs_ref[:, part:], wr_ref[:, cut], preferred_element_type=F32)
            for i in range(2):
                total = acc[i * rows : (i + 1) * rows]
                if adds:
                    total += rest[i][:, cut].astype(F32)
                rest[len(adds) + i][:, cut] = total.astype(BF)
            return carry

        lax.fori_loop(0, cols // tile, columns, 0)

    def pick(at):
        return pl.BlockSpec((1, tokens, feats), lambda j: (at, 0, 0))

    w_spec = pl.BlockSpec((part, cols), lambda j: (0, 0))
    flat = pl.BlockSpec((rows, cols), lambda j: (0, 0))
    (one, at_one), (two, at_two) = groups
    return pl.pallas_call(
        body,
        out_shape=[jax.ShapeDtypeStruct((rows, cols), BF)] * 2,
        grid=(1,),
        in_specs=[SMEM, pick(at_one), pick(at_two), w_spec, w_spec] + [flat] * len(adds),
        out_specs=[flat, flat],
        scratch_shapes=[pltpu.VMEM((2 * rows, feats), BF)],
        compiler_params=params(22),
        cost_estimate=cost(4 * rows * feats * cols, 1e7),
        name="product",
    )(idx, one, two, w_own, w_recv, *adds)


def hidden_call(own, left, right):
    rows, cols = own[0].shape
    units = cols // 2

    def body(*refs):
        out_ref = refs[-1]
        for h in range(2):
            def both(cut):
                return sum(refs[2 * i + h][:, cut].astype(F32) for i in range(3))

            gate = both(slice(0, units))
            up = both(slice(units, cols))
            out_ref[h] = (gate / (1.0 + jnp.exp(-gate)) * up).astype(BF)

    return pl.pallas_call(
        body,
        out_shape=jax.ShapeDtypeStruct((2, rows, units), BF),
        in_specs=[VMEM] * 6,
        out_specs=VMEM,
        compiler_params=params(10),
        cost_estimate=cost(1e9, 4e6),
        name="hidden",
    )(*own, *left, *right)


def cut_half(array, at):
    _, rows, cols = array.shape

    def body(in_ref, out_ref):
        out_ref[...] = in_ref[0]

    return pl.pallas_call(
        body,
        out_shape=jax.ShapeDtypeStruct((rows, cols), array.dtype),
        grid=(1,),
        in_specs=[pl.BlockSpec((1, rows, cols), lambda j: (at, 0, 0))],
        out_specs=pl.BlockSpec((rows, cols), lambda j: (0, 0)),
        compiler_params=params(2),
        cost_estimate=cost(1e7, 4e5),
        name="cut_half",
    )(array)


def down_call(idx, dists, mine, theirs, weight, to_hbm):
    head = mine[0][0]
    rows, units = (head[0] if isinstance(head, tuple) else head).shape[-2:]
    cols = weight.shape[1]
    quarter = rows // 2
    sources = [pair for both in zip(mine, theirs) for pair in both]
    flat, places = [], []
    for pair in sources:
        for item in pair:
            array, at = item if isinstance(item, tuple) else (item, None)
            if not any(array is f for f in flat):
                flat.append(array)
            places.append((next(i for i, f in enumerate(flat) if f is array), at))
    n_in = len(flat)

    def body(idx_ref, *refs):
        w_ref = refs[n_in]
        out_ref, sq_ref, lhs_ref = refs[-3:]
        x = idx_ref[0]
        c = idx_ref[1]

        def load(n):
            i, at = places[n]
            return refs[i][...] if at is None else refs[i][at]

        halves = (c, 1 - c)

        @pl.when(pl.program_id(0) == 0)
        def _():
            for i, d in enumerate(dists):
                chip = lax.rem(x + 4 - d, 4)
                for u in range(2):
                    for s in range(2):
                        v = load(4 * i + 2 * u + s)
                        at = (2 * i + s) * rows
                        lhs_ref[at : at + rows, u * units : (u + 1) * units] = v
                        v = v.astype(F32)
                        cut = pl.ds(pl.multiple_of(halves[u] * units, 128), units)
                        sq_ref[2 * chip + halves[s], :, cut] = jnp.sum(
                            (v * v).reshape(-1, 8, units), axis=0
                        )

        own_rows = pl.ds(pl.multiple_of(c * units, 128), units)
        other_rows = pl.ds(pl.multiple_of((1 - c) * units, 128), units)
        acc = jnp.dot(lhs_ref[:, :units], w_ref[own_rows, :], preferred_element_type=F32)
        acc += jnp.dot(lhs_ref[:, units:], w_ref[other_rows, :], preferred_element_type=F32)
        out = acc.astype(BF)
        for i, d in enumerate(dists):
            z = lax.rem(x + 4 - d, 4)
            for s in range(2):
                for h in range(2):
                    lo = (2 * i + s) * rows + h * quarter
                    out_ref[4 * z + 2 * halves[s] + h] = out[lo : lo + quarter]

    def whole(a):
        return pl.BlockSpec(a.shape, lambda i, idx_ref: (0,) * a.ndim)

    out_shape = [
        (pltpu.HBM if to_hbm else jax.ShapeDtypeStruct)((16, quarter, cols), BF),
        jax.ShapeDtypeStruct((8, 8, 2 * units), F32),
    ]
    args = [*flat, weight]
    return pl.pallas_call(
        body,
        out_shape=out_shape,
        grid_spec=pltpu.PrefetchScalarGridSpec(
            num_scalar_prefetch=1,
            grid=(cols // DOWN_TILE,),
            in_specs=[whole(a) for a in flat]
            + [pl.BlockSpec((2 * units, DOWN_TILE), lambda i, idx_ref: (0, i))],
            out_specs=[
                pl.BlockSpec((16, quarter, DOWN_TILE), lambda i, idx_ref: (0, 0, i)),
                whole(out_shape[1]),
            ],
            scratch_shapes=[pltpu.VMEM((2 * len(dists) * rows, 2 * units), BF)],
        ),
        compiler_params=params(20),
        cost_estimate=cost(1e9 * len(dists), 8e6),
        name="down",
    )(idx, *args)


def last_block(idx_ref, pairs, w_ref, sq_ref, lhs_ref, block_ref):
    rows, units = pairs[0][0].shape
    quarter = rows // 2
    c = idx_ref[1]
    cores = (c, 1 - c)
    for u, pair in enumerate(pairs):
        cut = pl.ds(pl.multiple_of(cores[u] * units, 128), units)
        for s in range(2):
            v = pair[s][...]
            lhs_ref[s * rows : (s + 1) * rows, u * units : (u + 1) * units] = v
            v = v.astype(F32)
            sq_ref[cores[s], :, cut] = jnp.sum((v * v).reshape(-1, 8, units), axis=0)
    own_rows = pl.ds(pl.multiple_of(c * units, 128), units)
    other_rows = pl.ds(pl.multiple_of((1 - c) * units, 128), units)
    acc = jnp.dot(lhs_ref[:, :units], w_ref[own_rows, :], preferred_element_type=F32)
    acc += jnp.dot(lhs_ref[:, units:], w_ref[other_rows, :], preferred_element_type=F32)
    out = acc.astype(BF)
    for s in range(2):
        for h in range(2):
            lo = s * rows + h * quarter
            block_ref[2 * cores[s] + h] = out[lo : lo + quarter]


def patch_call(idx, mine, theirs, weight, part):
    rows, units = mine[0].shape
    cols = weight.shape[1]

    def body(idx_ref, ma, mb, ta, tb, w_ref, out_in, sq_in, out_ref, sq_ref, lhs_ref):
        del out_in, sq_in
        last_block(idx_ref, ((ma, mb), (ta, tb)), w_ref, sq_ref, lhs_ref, out_ref)

    def whole(a):
        return pl.BlockSpec(a.shape, lambda i, idx_ref: (0,) * a.ndim)

    def place(i, idx_ref):
        return (lax.rem(idx_ref[0] + 2, 4), 0, 0)

    args = [*mine, *theirs, weight]
    return pl.pallas_call(
        body,
        out_shape=[
            pltpu.HBM((16, rows // 2, cols), BF),
            jax.ShapeDtypeStruct((8, 8, 2 * units), F32),
        ],
        grid_spec=pltpu.PrefetchScalarGridSpec(
            num_scalar_prefetch=1,
            grid=(1,),
            in_specs=[whole(a) for a in args] + [pl.BlockSpec(memory_space=pl.ANY)] * 2,
            out_specs=[
                pl.BlockSpec((4, rows // 2, cols), place),
                pl.BlockSpec((2, 8, 2 * units), place),
            ],
            scratch_shapes=[pltpu.VMEM((2 * rows, 2 * units), BF)],
        ),
        input_output_aliases={6: 0, 7: 1},
        compiler_params=params(20),
        cost_estimate=cost(1e9, 8e6),
        name="patch",
    )(idx, *args, in_hbm(part[0]), part[1])


def tail_call(idx, mine, theirs, weight, part):
    rows, units = mine[0].shape
    cols = weight.shape[1]
    quarter = rows // 2
    half = cols // 2

    def body(idx_ref, ma, mb, ta, tb, w_ref, part_ref, sq_in, *refs):
        del sq_in
        by_z, by_y = refs[0:4], refs[4:8]
        sq_ref, lhs_ref, block_ref = refs[8:]
        x, z, y = (idx_ref[i] for i in (0, 2, 3))
        last_block(idx_ref, ((ma, mb), (ta, tb)), w_ref, sq_ref, lhs_ref, block_ref)
        last = lax.rem(x + 2, 4)
        for e in range(4):
            to_z = lax.rem(z + e, 4)

            @pl.when(to_z == last)
            def _():
                by_z[e][...] = block_ref[:, :, :half]

            @pl.when(to_z != last)
            def _():
                by_z[e][...] = part_ref[pl.ds(4 * to_z, 4), :, :half]

            to_y = lax.rem(y + e, 4)
            for i in range(4):
                by_y[e][i] = part_ref[4 * i + to_y, :, half:]
            by_y[e][last] = block_ref[to_y, :, half:]

    def whole(a):
        return pl.BlockSpec(a.shape, lambda i, idx_ref: (0,) * len(a.shape))

    cut = jax.ShapeDtypeStruct((4, quarter, half), BF)
    args = [*mine, *theirs, weight, *part]
    res = pl.pallas_call(
        body,
        out_shape=[cut] * 8 + [jax.ShapeDtypeStruct((8, 8, 2 * units), F32)],
        grid_spec=pltpu.PrefetchScalarGridSpec(
            num_scalar_prefetch=1,
            grid=(1,),
            in_specs=[whole(a) for a in args[:-1]] + [pl.BlockSpec(memory_space=pl.ANY)],
            out_specs=[whole(cut)] * 8
            + [pl.BlockSpec((2, 8, 2 * units), lambda i, r: (lax.rem(r[0] + 2, 4), 0, 0))],
            scratch_shapes=[
                pltpu.VMEM((2 * rows, 2 * units), BF),
                pltpu.VMEM((4, quarter, cols), BF),
            ],
        ),
        input_output_aliases={7: 8},
        compiler_params=params(20),
        cost_estimate=cost(1e9, 8e6),
        name="tail",
    )(idx, *args)
    return res[:4], res[4:8], res[8]


def phase_sum(idx, axis, pieces):
    _, rows, cols = pieces[0].shape

    def body(idx_ref, *refs):
        ins, outs = refs[:4], refs[4:]
        for e in range(4):
            to = lax.rem(idx_ref[axis] + e, 4)
            outs[e][...] = sum(ref[to].astype(F32) for ref in ins).astype(BF)

    return pl.pallas_call(
        body,
        out_shape=[jax.ShapeDtypeStruct((rows, cols), BF)] * 4,
        in_specs=[SMEM] + [VMEM] * 4,
        out_specs=[VMEM] * 4,
        compiler_params=params(6),
        cost_estimate=cost(1e8, 2e6),
        name="phase_sum",
    )(idx, *pieces)


def final_sum(first, left, right):
    rows, cols = left[0].shape
    top = first.shape[0]

    def body(f_ref, *refs):
        out_ref = refs[-1]
        out_ref[:top] = f_ref[...]
        for i in range(2):
            total = sum(ref[...].astype(F32) for ref in refs[4 * i : 4 * i + 4])
            out_ref[top:, i * cols : (i + 1) * cols] = total.astype(BF)

    return pl.pallas_call(
        body,
        out_shape=jax.ShapeDtypeStruct((top + rows, 2 * cols), BF),
        in_specs=[VMEM] * 9,
        out_specs=VMEM,
        compiler_params=params(4),
        cost_estimate=cost(1e8, 2e6),
        name="final_sum",
    )(first, *left, *right)


def column_squares(idx, arrays):
    part = arrays[0].shape[2] // 2

    def body(*refs):
        total = jnp.zeros((8, part), F32)
        for ref in refs[1:-1]:
            for i in range(ref.shape[0]):
                v = ref[i].astype(F32)
                v = (v * v).reshape(-1, 8, part)
                total += jnp.sum(v, axis=0)
        refs[-1][...] = jnp.sum(total, axis=0, keepdims=True)

    def spec(a):
        return pl.BlockSpec((a.shape[0], a.shape[1], part), lambda i, idx_ref: (0, 0, idx_ref[1]))

    return pl.pallas_call(
        lambda *refs: body(*refs),
        out_shape=jax.ShapeDtypeStruct((1, part), F32),
        grid_spec=pltpu.PrefetchScalarGridSpec(
            num_scalar_prefetch=1,
            grid=(1,),
            in_specs=[spec(a) for a in arrays],
            out_specs=pl.BlockSpec((1, part), lambda i, idx_ref: (0, 0)),
        ),
        compiler_params=params(14),
        cost_estimate=cost(1e9, 4e6),
        name="squares",
    )(idx, *arrays)


def summed(parts):
    count, rows, cols = parts.shape
    tile = cols // 4

    def body(p_ref, out_ref):
        total = p_ref[0].astype(F32)
        for i in range(1, count):
            total += p_ref[i].astype(F32)
        out_ref[...] = total.astype(BF)

    return pl.pallas_call(
        body,
        out_shape=jax.ShapeDtypeStruct((rows, cols), BF),
        grid=(4,),
        in_specs=[pl.BlockSpec((count, rows, tile), lambda j: (0, 0, j))],
        out_specs=pl.BlockSpec((rows, tile), lambda j: (0, j)),
        compiler_params=params(8),
        cost_estimate=cost(1e8, 4e6),
        name="summed",
    )(parts)


def step(
    tokens, norm_gain, gate_weight, gate_mask, up_weight, up_mask, down_weight, down_mask
):
    idx = jnp.stack([lax.axis_index(a) for a in ("x", "c", "z", "y")]).astype(jnp.int32)
    (two,) = norm_call(idx, tokens, norm_gain, (2,), 2)
    one, three = norm_call(idx, tokens, norm_gain, (1, 3), 3)
    (own_x,) = norm_call(idx, tokens, norm_gain, (0,))
    own_x = own_x[None]
    got = {d: shift(v, "x", d) for d, v in ((2, two), (1, one), (3, three))}
    own_theirs = swap(own_x)
    w_own, w_send = mask_pair(idx, gate_weight, gate_mask, up_weight, up_mask)
    w_recv = swap(w_send)
    far = [got[2]] + [shift(got[2], "z", e) for e in (1, 2, 3)]
    near = jnp.stack([got[1], got[3]])
    near = [near] + [shift(near, "y", e) for e in (1, 2, 3)]
    far = assemble(idx, 2, far)
    far_theirs = swap(far)
    near = assemble(idx, 3, near)
    near_theirs = swap(near)
    down_kept = mask_one(down_weight, down_mask)

    tiles = (FULL_TILE, SMALL_TILE)
    hid = []
    for k in range(len(SPLIT)):
        w = (w_own, w_recv)
        far_a, far_b = product(idx, k, tiles[k], ((far, 0), (far_theirs, 0)), *w)
        from_left = shift(far_a, "x", 1)
        from_right = shift(far_b, "x", 3)
        groups = ((near_theirs, 1), (near, 0))
        free_b, free_a = product(idx, k, tiles[k], groups, *w)
        left_b = shift(free_b, "x", 1)
        right_a = shift(free_a, "x", 3)
        groups = ((own_x, 0), (own_theirs, 0))
        own = product(idx, k, SMALL_TILE, groups, *w)
        groups = ((near, 1), (near_theirs, 0))
        sums = (from_left, from_right)
        bound_a, bound_b = product(idx, k, tiles[k], groups, *w, sums)
        left_a = shift(bound_a, "x", 1)
        right_b = shift(bound_b, "x", 3)
        hid.append(hidden_call(own, (left_a, left_b), (right_a, right_b)))
    squares = []
    for k in range(len(SPLIT)):
        h0 = hid[k]
        h1 = shift(h0, "x", 1)
        h3 = shift(h0, "x", 3)
        h2a = shift(cut_half(h1, 0), "x", 1)
        h2b = shift(cut_half(h3, 1), "x", 3)
        p0, p1, p3 = swap(h0), swap(h1), swap(h3)
        p2a, p2b = swap(h2a), swap(h2b)
        mine = [((h, 0), (h, 1)) for h in (h0, h1, h3)]
        theirs = [((p, 1), (p, 0)) for p in (p0, p1, p3)]
        at_first = in_vmem(down_kept) if k == 0 else in_hbm(down_kept)
        part = down_call(idx, (0, 1, 3), mine, theirs, at_first, k == 0)
        if k == 0:
            out, sq = patch_call(idx, (h2a, h2b), (p2b, p2a), down_kept, part)
            parts = lax.all_to_all(out, MP, 0, 0, tiled=True).reshape(out.shape)
            mixed = summed(parts)
        else:
            by_z, by_y, sq = tail_call(idx, (h2a, h2b), (p2b, p2a), down_kept, part)
            by_z = [by_z[0]] + [shift(by_z[e], "z", e) for e in (1, 2, 3)]
            by_y = [by_y[0]] + [shift(by_y[e], "y", e) for e in (1, 2, 3)]
            left = phase_sum(idx, 3, by_z)
            left = [left[0]] + [shift(left[e], "y", e) for e in (1, 2, 3)]
            right = phase_sum(idx, 2, by_y)
            right = [right[0]] + [shift(right[e], "z", e) for e in (1, 2, 3)]
            mixed = final_sum(mixed, left, right)
        squares.append(sq)

    sums = column_squares(idx, [own_x, own_theirs, far, far_theirs, near, near_theirs])
    input_norms = jnp.sqrt(sums[0])
    hidden_norms = jnp.sqrt(jnp.sum(squares[0] + squares[1], axis=(0, 1)))
    return (mixed, input_norms, hidden_norms)


def solution(mesh):
    finer = Mesh(mesh.devices.reshape(4, 2, 4, 4), DP + MP)
    in_specs = (
        P(DP, None),
        P(),
        P(DP, MP),
        P(DP, MP),
        P(DP, MP),
        P(DP, MP),
        P(MP, DP),
        P(MP, DP),
    )
    out_specs = (P(MP, DP), P(DP), P(MP))
    return jax.shard_map(step, mesh=finer, in_specs=in_specs, out_specs=out_specs, check_vma=False)
```
